32 devices in a mesh: grp: 8 (over z, x), node: 4 (over y, core).
Axes of the slice: x: 2, y: 2, z: 4, core: 2. Of those that a mesh axis runs over, the one named last changes fastest.
Arguments:
- initial: float32 [6, 32, 32768], P(None, None, ('grp', 'node')), may hold values from -0.5 to 16, as said below
- afferent_noise_level: float32 [32, 32768], P(None, ('grp', 'node')), may hold values from 0.12 to 0.32
- history: bfloat16 [64, 32, 32768], P(None, None, ('grp', 'node')), may hold values from 0 to 1
- weights: bfloat16 [32, 24, 128, 1024], P(('grp', 'node')), may hold values from -0.109375 to 0.109375
- lead_field: bfloat16 [128, 32768], P(None, ('grp', 'node')), may hold values from -0.00390625 to 0.00390625
- src_group: int32 [32, 24], replicated, may hold values from 0 to 7, as said below
- src_sub: int32 [32, 24], replicated, may hold values from 0 to 7
- delays: int32 [32, 24], replicated, may hold values from 6 to 63
- counts: int32 [32], replicated, may hold values from 16 to 24, as said below
Outputs:
- final_state: float32 [6, 32, 32768], P(None, None, ('grp', 'node'))
- sensors: float32 [6, 128, 32], replicated
The draws below stay inside these ranges and needn't reach their ends.
Inputs may be any that keep to these rules, and one draw needn't show every extreme that they name: `initial`: rows 0 to 2 are potentials and rows 3 to 5 their rates; row 0 lies within 0 and 0.4, row 1 within 4 and 16, row 2 within 0 and 8, rows 3 to 5 within -0.5 and 0.5. `src_group`: among the tiles k < counts[b] of a block b no owner group appears more than 3 times, and some block reaches 3. Tiles k >= counts[b] of block b are ignored; in every draw some block has 24 live tiles.
All inputs are finite; a program needn't handle non-finite values.
Results may differ from the reference program's by a relative error of at most 0.0003.
The reference program's roundings to bfloat16 on the way (of `cycle` and `potential`) count: a program that leaves them out, or rounds other values in their place, can miss the bound.
Values may be sent and summed in bfloat16 or wider, within the bound.
A program may use at most 128 MiB of HBM per device.

```python
import math
import jax
import jax.numpy as jnp
from jax import lax

BLOCK = 1024
SUB = 128
KMAX = 24
CYCLE = 64
DMIN = 6
STEPS = 6
SENS = 128
REPS = 32
OWNERS = 8
COLUMNS = 4
BLOCKS = 32
NODES = 32768
CAP = 3
PIECES = 8


def draw_initial(key, part):
    keys = jax.random.split(key, 6)
    shape = (REPS, NODES)
    lows = (0.0, 4.0, 0.0, -0.5, -0.5, -0.5)
    highs = (0.4, 16.0, 8.0, 0.5, 0.5, 0.5)
    rows = []
    for row_index in range(6):
        unit = jax.random.uniform(keys[row_index], shape, jnp.float32)
        rows.append(lows[row_index] + (highs[row_index] - lows[row_index]) * unit)
    return jnp.stack(rows)


def draw_src_group(key, part):
    keys = jax.random.split(key, BLOCKS)

    def one_row(row_key):
        order = jax.random.permutation(row_key, CAP * OWNERS)
        return (order[:KMAX] % OWNERS).astype(jnp.int32)
    return jax.vmap(one_row)(keys)


def draw_counts(key, part):
    first_key, second_key = jax.random.split(key)
    base_counts = jax.random.randint(first_key, (BLOCKS,), KMAX - KMAX // 3, KMAX + 1)
    full_block = jax.random.randint(second_key, (), 0, BLOCKS)
    return base_counts.at[full_block].set(KMAX).astype(jnp.int32)


def place_ends(array, own_key, smallest, top_value):
    longest = array.shape.index(max(array.shape))
    spots = []
    for shift in (0, 1):
        where = [jax.random.randint(jax.random.fold_in(own_key, axis), (), 0, length) for axis, length in enumerate(array.shape)]
        where[longest] = (where[longest] + shift) % array.shape[longest]
        spots.append(tuple(where))
    return array.at[spots[0]].set(smallest).at[spots[1]].set(top_value)


def levels(own_key, extent, cuts, smallest, largest):
    def one(position, blocks):
        heights = jax.random.uniform(jax.random.fold_in(jax.random.fold_in(own_key, 6), position), (blocks,), jnp.float32, smallest / len(cuts), largest / len(cuts))
        return jnp.repeat(jnp.exp(heights), extent[position] // blocks).reshape((-1,) + (1,) * (len(extent) - position - 1))

    loudness = one(*cuts[0])
    for cut in cuts[1:]:
        loudness = loudness * one(*cut)
    return loudness


def gaussian(own_key, dims, width, limit, cuts=(), kind=jnp.bfloat16):
    drawn = width * jax.random.normal(own_key, dims, jnp.float32)
    if cuts:
        drawn = drawn * levels(own_key, dims, cuts, -0.22, 0.18)
    return jnp.clip(drawn, -limit, limit).astype(kind)


def setup_inputs(seed: int = 0) -> dict:
    splits = jax.random.split(jax.random.key(seed), 10)
    initial = draw_initial(jax.random.fold_in(splits[9], 71), 0)
    afferent_noise_level = jnp.clip(jnp.exp(math.log(0.32) - 0.98082925 * jax.random.uniform(splits[1], (REPS, NODES), jnp.float32) ** levels(splits[1], (REPS, NODES), ((1, 32),), -0.2, 0.2)), 0.12, 0.32)
    history = jnp.clip(1.0 * jax.random.uniform(splits[2], (CYCLE, REPS, NODES), jnp.float32) ** levels(splits[2], (CYCLE, REPS, NODES), ((2, 32),), -0.2, 0.2), 0.0, 1.0).astype(jnp.bfloat16)
    weights = gaussian(splits[3], (BLOCKS, KMAX, SUB, BLOCK), (KMAX * SUB) ** -0.5, 0.109375, ((0, 32),))
    lead_field = gaussian(splits[4], (SENS, NODES), (64 * NODES) ** -0.5, 0.00390625, ((1, 32),))
    src_group = draw_src_group(jax.random.fold_in(splits[9], 71), 0)
    src_sub = place_ends(jax.random.randint(splits[6], (BLOCKS, KMAX), 0, PIECES), jax.random.fold_in(splits[6], 1), 0, PIECES - 1).astype(jnp.int32)
    delays = place_ends(jax.random.randint(splits[7], (BLOCKS, KMAX), DMIN, CYCLE), jax.random.fold_in(splits[7], 1), DMIN, CYCLE - 1).astype(jnp.int32)
    counts = draw_counts(jax.random.fold_in(splits[9], 71), 0)
    return dict(initial=initial, afferent_noise_level=afferent_noise_level, history=history, weights=weights, lead_field=lead_field, src_group=src_group, src_sub=src_sub, delays=delays, counts=counts)


exciting_amplitude = 3.25
suppressive_amplitude = 22.0
exciting_inverse_lag = 0.1
suppressive_inverse_lag = 0.05
link_factor = 135.0
maximal_spike_frequency = 0.005
thresh = 6.0
fire_slope = 0.56
global_scaling_factor = 0.5
dt_step = 0.5


def sigmoid_spike_density(somatic_charge_level):
    return 1.0 / (1.0 + jnp.exp(fire_slope * (thresh - somatic_charge_level)))


def derivative(population_variables, afferent_noise_level, network_afferent):
    principal_cell_level, interneuron_depolarization, suppressive_depolarization = population_variables[0], population_variables[1], population_variables[2]
    principal_cell_curvature = exciting_amplitude * exciting_inverse_lag * maximal_spike_frequency * sigmoid_spike_density(interneuron_depolarization - suppressive_depolarization) - 2.0 * exciting_inverse_lag * population_variables[3] - exciting_inverse_lag * exciting_inverse_lag * principal_cell_level
    interneuron_second_derivative = exciting_amplitude * exciting_inverse_lag * (afferent_noise_level + 0.8 * link_factor * maximal_spike_frequency * sigmoid_spike_density(link_factor * principal_cell_level) + global_scaling_factor * network_afferent) - 2.0 * exciting_inverse_lag * population_variables[4] - exciting_inverse_lag * exciting_inverse_lag * interneuron_depolarization
    suppressive_second_derivative = suppressive_amplitude * suppressive_inverse_lag * 0.25 * link_factor * maximal_spike_frequency * sigmoid_spike_density(0.25 * link_factor * principal_cell_level) - 2.0 * suppressive_inverse_lag * population_variables[5] - suppressive_inverse_lag * suppressive_inverse_lag * suppressive_depolarization
    return jnp.stack([population_variables[3], population_variables[4], population_variables[5], principal_cell_curvature, interneuron_second_derivative, suppressive_second_derivative])


def advance(population_variables, afferent_noise_level, coupled_now, coupled_next):
    first_rate = derivative(population_variables, afferent_noise_level, coupled_now)
    second_rate = derivative(population_variables + dt_step * first_rate, afferent_noise_level, coupled_next)
    return population_variables + (0.5 * dt_step) * (first_rate + second_rate)


def gather_input(cycle, in_time, weights, src_group, src_sub, delays, counts):
    zero_index = jnp.zeros((), jnp.int32)
    tile_lanes = jnp.arange(KMAX, dtype=jnp.int32)
    column = jnp.arange(BLOCKS, dtype=jnp.int32) % COLUMNS
    starts = ((src_group * COLUMNS + column[:, None]) * BLOCK + src_sub * SUB).astype(jnp.int32)
    slot_ids = jnp.mod(in_time - delays, CYCLE).astype(jnp.int32)

    def cut_piece(slot_id, start_id):
        return lax.dynamic_slice(cycle, (slot_id, zero_index, start_id), (1, REPS, SUB))[0]

    def one_block(element):
        start_row, slot_row, live_count, tile_block = element
        pieces = jax.vmap(cut_piece)(slot_row, start_row)
        live_mask = (tile_lanes < live_count).astype(jnp.bfloat16)
        pieces = pieces * live_mask[:, None, None]
        flattened = jnp.transpose(pieces, (1, 0, 2)).reshape(REPS, KMAX * SUB)
        return jnp.dot(flattened, tile_block.reshape(KMAX * SUB, BLOCK), preferred_element_type=jnp.float32)

    products = lax.map(one_block, (starts, slot_ids, counts, weights), batch_size=8)
    return jnp.transpose(products, (1, 0, 2)).reshape(REPS, BLOCKS * BLOCK)


def reference(initial, afferent_noise_level, history, weights, lead_field, src_group, src_sub, delays, counts):
    zero_index = jnp.zeros((), jnp.int32)

    def inputs(cycle, in_time):
        return gather_input(cycle, in_time, weights, src_group, src_sub, delays, counts)

    def record(sensors, population_variables, step_id):
        potential = (population_variables[1] - population_variables[2]).astype(jnp.bfloat16)
        local_sum = lax.dot_general(lead_field, potential, (((1,), (1,)), ((), ())), preferred_element_type=jnp.float32)
        return lax.dynamic_update_slice(sensors, local_sum[None], (step_id, zero_index, zero_index))

    network_afferent = inputs(history, jnp.zeros((), jnp.int32))
    sensors = jnp.zeros((STEPS, SENS, REPS), jnp.float32)

    def one_step(step_id, carried):
        population_variables, cycle, coupled_now, sensors = carried
        step_id = jnp.asarray(step_id).astype(jnp.int32)
        spike_density_result = sigmoid_spike_density(population_variables[1] - population_variables[2]).astype(jnp.bfloat16)
        cycle = lax.dynamic_update_slice(cycle, spike_density_result[None], (jnp.mod(step_id, CYCLE).astype(jnp.int32), zero_index, zero_index))
        coupled_next = inputs(cycle, step_id + 1)
        population_variables = advance(population_variables, afferent_noise_level, coupled_now, coupled_next)
        return population_variables, cycle, coupled_next, record(sensors, population_variables, step_id)

    population_variables, cycle, network_afferent, sensors = lax.fori_loop(0, STEPS, one_step, (initial, history, network_afferent, sensors))
    return population_variables, sensors
```

```python
import functools

import jax
import jax.numpy as jnp
from jax import lax
from jax.experimental import pallas as pl
from jax.experimental.pallas import tpu as pltpu
from jax.sharding import PartitionSpec as P

DMIN = 6
STEPS = 6
TIME_GROUPS = ((0, 1), (2, 3), (4, 5), (6,))

exciting_amplitude = 3.25
suppressive_amplitude = 22.0
exciting_inverse_lag = 0.1
suppressive_inverse_lag = 0.05
link_factor = 135.0
maximal_spike_frequency = 0.005
thresh = 6.0
fire_slope = 0.56
global_scaling_factor = 0.5
dt_step = 0.5

MESH = pl.DeviceIdType.MESH


def sigmoid_spike_density(level):
    return 1.0 / (1.0 + jnp.exp(fire_slope * (thresh - level)))


def derivative(y, noise, coupled):
    curvature = (
        exciting_amplitude
        * exciting_inverse_lag
        * maximal_spike_frequency
        * sigmoid_spike_density(y[1] - y[2])
        - 2.0 * exciting_inverse_lag * y[3]
        - exciting_inverse_lag * exciting_inverse_lag * y[0]
    )
    interneuron = (
        exciting_amplitude
        * exciting_inverse_lag
        * (
            noise
            + 0.8
            * link_factor
            * maximal_spike_frequency
            * sigmoid_spike_density(link_factor * y[0])
            + global_scaling_factor * coupled
        )
        - 2.0 * exciting_inverse_lag * y[4]
        - exciting_inverse_lag * exciting_inverse_lag * y[1]
    )
    suppressive = (
        suppressive_amplitude
        * suppressive_inverse_lag
        * 0.25
        * link_factor
        * maximal_spike_frequency
        * sigmoid_spike_density(0.25 * link_factor * y[0])
        - 2.0 * suppressive_inverse_lag * y[5]
        - suppressive_inverse_lag * suppressive_inverse_lag * y[2]
    )
    return [y[3], y[4], y[5], curvature, interneuron, suppressive]


def advance(y, noise, coupled_now, coupled_next):
    first = derivative(y, noise, coupled_now)
    moved = [a + dt_step * b for a, b in zip(y, first)]
    second = derivative(moved, noise, coupled_next)
    return [a + 0.5 * dt_step * (b + c) for a, b, c in zip(y, first, second)]


def pack_kernel(
    owners,
    columns,
    slots,
    src_group,
    src_sub,
    delays,
    counts,
    initial,
    hist,
    own_place,
    *rest,
):
    groups = len(TIME_GROUPS)
    packed = rest[:groups]
    sel_sub, sel_delay, fired = rest[groups:]
    me = lax.axis_index("grp")
    column = lax.axis_index("node")
    cycle_len, replicas, block_len = hist.shape
    tiles = src_group.shape[0]
    piece_len = packed[0].shape[3]

    def choose(dest, carry):
        block = dest * columns + column
        live = counts[block]
        rank = jnp.int32(0)
        subs = [jnp.int32(0)] * slots
        waits = [jnp.int32(DMIN)] * slots
        for k in range(tiles):
            hit = jnp.logical_and(src_group[k, block] == me, k < live)
            sub, wait = src_sub[k, block], delays[k, block]
            for r in range(slots):
                take = jnp.logical_and(hit, rank == r)
                subs[r] = jnp.where(take, sub, subs[r])
                waits[r] = jnp.where(take, wait, waits[r])
            rank = rank + jnp.where(hit, 1, 0)
        for r in range(slots):
            sel_sub[dest * slots + r] = subs[r]
            sel_delay[dest * slots + r] = waits[r]
        return carry

    lax.fori_loop(0, owners, choose, 0)

    my_block = me * columns + column
    my_live = counts[my_block]
    my_groups = [src_group[k, my_block] for k in range(tiles)]
    for k in range(tiles):
        rank = jnp.int32(0)
        for earlier in range(k):
            rank = rank + jnp.where(my_groups[earlier] == my_groups[k], 1, 0)
        place = my_groups[k] * slots + jnp.minimum(rank, slots - 1)
        own_place[k] = jnp.where(k < my_live, place, owners * slots)

    def first_fire(tile, carry):
        cols = pl.ds(pl.multiple_of(tile * piece_len, piece_len), piece_len)
        fire = sigmoid_spike_density(initial[1, :, cols] - initial[2, :, cols])
        fired[:, cols] = fire.astype(jnp.bfloat16)
        return carry

    lax.fori_loop(0, block_len // piece_len, first_fire, 0)

    def pack(place, carry):
        start = cycle_len - sel_delay[place]
        cols = pl.ds(pl.multiple_of(sel_sub[place] * piece_len, piece_len), piece_len)
        for times, parcel in zip(TIME_GROUPS, packed):
            for j, t in enumerate(times):
                if t < DMIN:
                    parcel[place, j] = hist[start + t, :, cols]
                else:
                    past = hist[jnp.minimum(start + t, cycle_len - 1), :, cols]
                    parcel[place, j] = jnp.where(start + t < cycle_len, past, fired[:, cols])
        return carry

    lax.fori_loop(0, owners * slots, pack, 0)


def kernel(
    owners,
    columns,
    slots,
    own_place,
    initial,
    noise,
    weights,
    lead,
    *rest,
):
    group_count = len(TIME_GROUPS)
    packed = rest[:group_count]
    landed = rest[-group_count:]
    run(owners, columns, slots, own_place, initial, noise, weights, lead, packed, landed, *rest[group_count:-group_count])


def run(
    owners,
    columns,
    slots,
    own_place,
    initial,
    noise,
    weights,
    lead,
    packed,
    landed,
    state,
    sensors_out,
    lhs,
    coupled,
    potential,
    partial,
    scatter_in,
    node_in,
    gathered,
    send_sem,
    recv_sem,
    scatter_send,
    scatter_recv,
    node_send,
    node_recv,
    gather_send,
    gather_recv,
):
    group_count = len(TIME_GROUPS)
    me = lax.axis_index("grp")
    column = lax.axis_index("node")
    replicas, block_len = noise.shape
    tiles = own_place.shape[0]
    piece_len = weights.shape[0] // tiles
    offsets = sorted(range(1, owners), key=lambda o: abs(2 * o - owners))

    barrier = pltpu.get_barrier_semaphore()
    for o in offsets:
        pl.semaphore_signal(
            barrier, inc=1, device_id={"grp": lax.rem(me + o, owners)}, device_id_type=MESH
        )
    for o in range(1, columns):
        pl.semaphore_signal(
            barrier, inc=1, device_id={"node": lax.rem(column + o, columns)}, device_id_type=MESH
        )

    mine = pl.ds(me * slots, slots)
    spare = owners * slots
    for g in range(group_count):
        landed[g][mine] = packed[g][mine]
        landed[g][spare] = jnp.zeros(landed[g].shape[1:], jnp.bfloat16)

    pl.semaphore_wait(barrier, owners + columns - 2)

    def parcel_copy(g, o):
        dest = lax.rem(me + o, owners)
        return pltpu.make_async_remote_copy(
            src_ref=packed[g].at[pl.ds(dest * slots, slots)],
            dst_ref=landed[g].at[mine],
            send_sem=send_sem.at[g, o],
            recv_sem=recv_sem.at[g, o],
            device_id={"grp": dest},
            device_id_type=MESH,
        )

    for g in range(group_count):
        for o in offsets:
            parcel_copy(g, o).start()

    dot_cols = min(256, block_len)
    rows_per = replicas
    chunk = partial.shape[1]

    for g, times in enumerate(TIME_GROUPS):
        for o in offsets:
            parcel_copy(g, o).wait_recv()
        rows = len(times) * rows_per
        base = times[0] * rows_per

        for k in range(tiles):
            piece = landed[g][own_place[k]]
            lhs[:rows, k * piece_len : (k + 1) * piece_len] = piece.reshape(rows, piece_len)

        def multiply(tile, carry):
            cols = pl.ds(pl.multiple_of(tile * dot_cols, dot_cols), dot_cols)
            coupled[base : base + rows, cols] = jnp.dot(
                lhs[:rows, :], weights[:, cols], preferred_element_type=jnp.float32
            )
            return carry

        lax.fori_loop(0, block_len // dot_cols, multiply, 0)

        steps = [t - 1 for t in times if t > 0]

        source = initial if g == 0 else state

        def move(tile, carry):
            cols = pl.ds(pl.multiple_of(tile * piece_len, piece_len), piece_len)
            y = [source[i, :, cols] for i in range(6)]
            drive = noise[:, cols]
            now = coupled[steps[0] * rows_per : (steps[0] + 1) * rows_per, cols]
            for i, s in enumerate(steps):
                later = coupled[(s + 1) * rows_per : (s + 2) * rows_per, cols]
                y = advance(y, drive, now, later)
                now = later
                potential[i * rows_per : (i + 1) * rows_per, cols] = (y[1] - y[2]).astype(
                    jnp.bfloat16
                )
            for i in range(6):
                state[i, :, cols] = y[i]
            return carry

        lax.fori_loop(0, block_len // piece_len, move, 0)

        signal = lax.dot_general(
            potential[: len(steps) * rows_per, :],
            lead[...],
            (((1,), (1,)), ((), ())),
            preferred_element_type=jnp.float32,
        )
        row = steps[0] * rows_per
        stop = row + len(steps) * rows_per
        first_row = row
        while row < stop:
            part, inside = divmod(row, chunk)
            many = min(chunk - inside, stop - row)
            partial[part, inside : inside + many, :] = signal[
                row - first_row : row - first_row + many, :
            ]
            row += many

    def scatter_copy(o):
        dest = lax.rem(me + o, owners)
        return pltpu.make_async_remote_copy(
            src_ref=partial.at[dest],
            dst_ref=scatter_in.at[o],
            send_sem=scatter_send.at[o],
            recv_sem=scatter_recv.at[o],
            device_id={"grp": dest},
            device_id_type=MESH,
        )

    for o in offsets:
        scatter_copy(o).start()
    for g in range(group_count):
        for o in offsets:
            parcel_copy(g, o).wait_send()
    total = partial[me]
    for o in reversed(offsets):
        scatter_copy(o).wait_recv()
        total = total + scatter_in[o]
    node_in[column] = total

    def node_copy(o):
        return pltpu.make_async_remote_copy(
            src_ref=node_in.at[column],
            dst_ref=node_in.at[column],
            send_sem=node_send.at[o],
            recv_sem=node_recv.at[o],
            device_id={"node": lax.rem(column + o, columns)},
            device_id_type=MESH,
        )

    for o in range(1, columns):
        node_copy(o).start()
    for o in range(1, columns):
        node_copy(o).wait_recv()
    total = node_in[0]
    for c in range(1, columns):
        total = total + node_in[c]
    gathered[me] = total

    def gather_copy(o):
        return pltpu.make_async_remote_copy(
            src_ref=gathered.at[me],
            dst_ref=gathered.at[me],
            send_sem=gather_send.at[o],
            recv_sem=gather_recv.at[o],
            device_id={"grp": lax.rem(me + o, owners)},
            device_id_type=MESH,
        )

    for o in offsets:
        gather_copy(o).start()
    for o in offsets:
        scatter_copy(o).wait_send()
    for o in range(1, columns):
        node_copy(o).wait_send()
    for o in offsets:
        gather_copy(o).wait_recv()
    sensors_out[...] = gathered[...]
    for o in offsets:
        gather_copy(o).wait_send()


def body(
    owners,
    columns,
    initial,
    afferent_noise_level,
    history,
    weights,
    lead_field,
    src_group,
    src_sub,
    delays,
    counts,
):
    cycle_len, replicas, block_len = history.shape
    tiles = src_group.shape[1]
    piece_len = weights.shape[2]
    sensors = lead_field.shape[0]
    slots = (tiles + owners - 1) // owners
    chunk = (STEPS * replicas + owners - 1) // owners
    groups = len(TIME_GROUPS)
    most = max(len(times) for times in TIME_GROUPS) * replicas
    smem = pl.BlockSpec(memory_space=pltpu.SMEM)
    vmem = pl.BlockSpec(memory_space=pltpu.VMEM)
    own_place, *packed = pl.pallas_call(
        functools.partial(pack_kernel, owners, columns, slots),
        out_shape=[jax.ShapeDtypeStruct((tiles,), jnp.int32)]
        + [
            jax.ShapeDtypeStruct(
                (owners * slots, len(times), replicas, piece_len), jnp.bfloat16
            )
            for times in TIME_GROUPS
        ],
        in_specs=[smem] * 4 + [vmem] * 2,
        out_specs=[smem] + [vmem] * groups,
        scratch_shapes=[
            pltpu.SMEM((owners * slots,), jnp.int32),
            pltpu.SMEM((owners * slots,), jnp.int32),
            pltpu.VMEM((replicas, block_len), jnp.bfloat16),
        ],
        compiler_params=pltpu.CompilerParams(vmem_limit_bytes=8 * 1024 * 1024),
        cost_estimate=pl.CostEstimate(flops=0, bytes_accessed=8 * 1024 * 1024, transcendentals=0),
    )(src_group.T, src_sub.T, delays.T, counts, initial, history)
    final, signal = pl.pallas_call(
        functools.partial(kernel, owners, columns, slots),
        out_shape=(
            jax.ShapeDtypeStruct(initial.shape, jnp.float32),
            jax.ShapeDtypeStruct((owners, chunk, sensors), jnp.float32),
        ),
        in_specs=[smem] + [vmem] * (4 + groups),
        out_specs=(vmem, vmem),
        scratch_shapes=[
            pltpu.VMEM((most, tiles * piece_len), jnp.bfloat16),
            pltpu.VMEM(((STEPS + 1) * replicas, block_len), jnp.float32),
            pltpu.VMEM((most, block_len), jnp.bfloat16),
            pltpu.VMEM((owners, chunk, sensors), jnp.float32),
            pltpu.VMEM((owners, chunk, sensors), jnp.float32),
            pltpu.VMEM((columns, chunk, sensors), jnp.float32),
            pltpu.VMEM((owners, chunk, sensors), jnp.float32),
            pltpu.SemaphoreType.DMA((groups, owners)),
            pltpu.SemaphoreType.DMA((groups, owners)),
            pltpu.SemaphoreType.DMA((owners,)),
            pltpu.SemaphoreType.DMA((owners,)),
            pltpu.SemaphoreType.DMA((columns,)),
            pltpu.SemaphoreType.DMA((columns,)),
            pltpu.SemaphoreType.DMA((owners,)),
            pltpu.SemaphoreType.DMA((owners,)),
        ]
        + [
            pltpu.VMEM((owners * slots + 1, len(times), replicas, piece_len), jnp.bfloat16)
            for times in TIME_GROUPS
        ],
        compiler_params=pltpu.CompilerParams(
            collective_id=0, has_side_effects=True, vmem_limit_bytes=20 * 1024 * 1024
        ),
    )(
        own_place,
        initial,
        afferent_noise_level,
        weights.reshape(tiles * piece_len, block_len),
        lead_field,
        *packed,
    )
    signal = signal.reshape(owners * chunk, sensors)[: STEPS * replicas]
    signal = signal.reshape(STEPS, replicas, sensors)
    return final, jnp.transpose(signal, (0, 2, 1))


def solution(mesh):
    return jax.shard_map(
        functools.partial(body, mesh.shape["grp"], mesh.shape["node"]),
        mesh=mesh,
        in_specs=(
            P(None, None, ("grp", "node")),
            P(None, ("grp", "node")),
            P(None, None, ("grp", "node")),
            P(("grp", "node"), None, None, None),
            P(None, ("grp", "node")),
            P(),
            P(),
            P(),
            P(),
        ),
        out_specs=(P(None, None, ("grp", "node")), P()),
        check_vma=False,
    )
```

```python
import functools

import jax
import jax.numpy as jnp
from jax import lax
from jax.experimental import pallas as pl
from jax.experimental.pallas import tpu as pltpu
from jax.sharding import PartitionSpec as P

DMIN = 6
STEPS = 6
VMEM_BYTES = 67043328
TIME_GROUPS = ((0, 1), (2, 3), (4, 5), (6,))

exciting_amplitude = 3.25
suppressive_amplitude = 22.0
exciting_inverse_lag = 0.1
suppressive_inverse_lag = 0.05
link_factor = 135.0
maximal_spike_frequency = 0.005
thresh = 6.0
fire_slope = 0.56
global_scaling_factor = 0.5
dt_step = 0.5

MESH = pl.DeviceIdType.MESH


def sigmoid_spike_density(level):
    return 1.0 / (1.0 + jnp.exp(fire_slope * (thresh - level)))


def derivative(y, noise, coupled):
    curvature = (
        exciting_amplitude
        * exciting_inverse_lag
        * maximal_spike_frequency
        * sigmoid_spike_density(y[1] - y[2])
        - 2.0 * exciting_inverse_lag * y[3]
        - exciting_inverse_lag * exciting_inverse_lag * y[0]
    )
    interneuron = (
        exciting_amplitude
        * exciting_inverse_lag
        * (
            noise
            + 0.8
            * link_factor
            * maximal_spike_frequency
            * sigmoid_spike_density(link_factor * y[0])
            + global_scaling_factor * coupled
        )
        - 2.0 * exciting_inverse_lag * y[4]
        - exciting_inverse_lag * exciting_inverse_lag * y[1]
    )
    suppressive = (
        suppressive_amplitude
        * suppressive_inverse_lag
        * 0.25
        * link_factor
        * maximal_spike_frequency
        * sigmoid_spike_density(0.25 * link_factor * y[0])
        - 2.0 * suppressive_inverse_lag * y[5]
        - suppressive_inverse_lag * suppressive_inverse_lag * y[2]
    )
    return [y[3], y[4], y[5], curvature, interneuron, suppressive]


def advance(y, noise, coupled_now, coupled_next):
    first = derivative(y, noise, coupled_now)
    moved = [a + dt_step * b for a, b in zip(y, first)]
    second = derivative(moved, noise, coupled_next)
    return [a + 0.5 * dt_step * (b + c) for a, b, c in zip(y, first, second)]


def pack_kernel(
    owners,
    columns,
    slots,
    src_group,
    src_sub,
    delays,
    counts,
    initial_hbm,
    history_hbm,
    own_place,
    *rest,
):
    groups = len(TIME_GROUPS)
    packed = rest[:groups]
    sel_sub, sel_delay, fired, fields, hist, local_sem = rest[groups:]
    me = lax.axis_index("grp")
    column = lax.axis_index("node")
    cycle_len, replicas, block_len = hist.shape
    tiles = src_group.shape[0]
    piece_len = packed[0].shape[3]

    load_fields = pltpu.make_async_copy(initial_hbm.at[pl.ds(1, 2)], fields, local_sem.at[0])
    load_history = pltpu.make_async_copy(history_hbm, hist, local_sem.at[1])
    load_fields.start()
    load_history.start()

    def choose(dest, carry):
        block = dest * columns + column
        live = counts[block]
        rank = jnp.int32(0)
        subs = [jnp.int32(0)] * slots
        waits = [jnp.int32(DMIN)] * slots
        for k in range(tiles):
            hit = jnp.logical_and(src_group[k, block] == me, k < live)
            sub, wait = src_sub[k, block], delays[k, block]
            for r in range(slots):
                take = jnp.logical_and(hit, rank == r)
                subs[r] = jnp.where(take, sub, subs[r])
                waits[r] = jnp.where(take, wait, waits[r])
            rank = rank + jnp.where(hit, 1, 0)
        for r in range(slots):
            sel_sub[dest * slots + r] = subs[r]
            sel_delay[dest * slots + r] = waits[r]
        return carry

    lax.fori_loop(0, owners, choose, 0)

    my_block = me * columns + column
    my_live = counts[my_block]
    my_groups = [src_group[k, my_block] for k in range(tiles)]
    for k in range(tiles):
        rank = jnp.int32(0)
        for earlier in range(k):
            rank = rank + jnp.where(my_groups[earlier] == my_groups[k], 1, 0)
        place = my_groups[k] * slots + jnp.minimum(rank, slots - 1)
        own_place[k] = jnp.where(k < my_live, place, owners * slots)

    load_fields.wait()

    def first_fire(tile, carry):
        cols = pl.ds(pl.multiple_of(tile * piece_len, piece_len), piece_len)
        fire = sigmoid_spike_density(fields[0, :, cols] - fields[1, :, cols])
        fired[:, cols] = fire.astype(jnp.bfloat16)
        return carry

    lax.fori_loop(0, block_len // piece_len, first_fire, 0)

    load_history.wait()

    def pack(place, carry):
        start = cycle_len - sel_delay[place]
        cols = pl.ds(pl.multiple_of(sel_sub[place] * piece_len, piece_len), piece_len)
        for times, parcel in zip(TIME_GROUPS, packed):
            for j, t in enumerate(times):
                if t < DMIN:
                    parcel[place, j] = hist[start + t, :, cols]
                else:
                    past = hist[jnp.minimum(start + t, cycle_len - 1), :, cols]
                    parcel[place, j] = jnp.where(start + t < cycle_len, past, fired[:, cols])
        return carry

    lax.fori_loop(0, owners * slots, pack, 0)


def kernel(
    owners,
    columns,
    slots,
    own_place,
    initial_hbm,
    noise_hbm,
    weights_hbm,
    lead_hbm,
    *rest,
):
    group_count = len(TIME_GROUPS)
    packed = rest[:group_count]
    landed = rest[-group_count:]
    staged = rest[-2 * group_count : -group_count]
    (
        final_hbm,
        sensors_out,
        state,
        noise,
        weights,
        lead,
        lhs,
        coupled,
        potential,
        partial,
        scatter_in,
        node_in,
        gathered,
        local_sem,
        keep_sem,
        stage_sem,
        send_sem,
        recv_sem,
        scatter_send,
        scatter_recv,
        node_send,
        node_recv,
        gather_send,
        gather_recv,
    ) = rest[group_count : -2 * group_count]
    me = lax.axis_index("grp")
    column = lax.axis_index("node")
    mine = pl.ds(me * slots, slots)
    stage = [
        pltpu.make_async_copy(packed[g], staged[g], stage_sem.at[g]) for g in range(group_count)
    ]
    for copy in stage:
        copy.start()
    replicas, block_len = noise.shape
    tiles = own_place.shape[0]
    piece_len = weights.shape[0] // tiles
    offsets = sorted(range(1, owners), key=lambda o: abs(2 * o - owners))

    barrier = pltpu.get_barrier_semaphore()
    for o in offsets:
        pl.semaphore_signal(
            barrier, inc=1, device_id={"grp": lax.rem(me + o, owners)}, device_id_type=MESH
        )
    for o in range(1, columns):
        pl.semaphore_signal(
            barrier, inc=1, device_id={"node": lax.rem(column + o, columns)}, device_id_type=MESH
        )

    spare = owners * slots
    for g in range(group_count):
        landed[g][spare] = jnp.zeros(landed[g].shape[1:], jnp.bfloat16)

    for copy in stage:
        copy.wait()
    keep = [
        pltpu.make_async_copy(packed[g].at[mine], landed[g].at[mine], keep_sem.at[g])
        for g in range(group_count)
    ]
    loads = [
        pltpu.make_async_copy(weights_hbm, weights, local_sem.at[0]),
        pltpu.make_async_copy(initial_hbm, state, local_sem.at[1]),
        pltpu.make_async_copy(noise_hbm, noise, local_sem.at[2]),
        pltpu.make_async_copy(lead_hbm, lead, local_sem.at[3]),
    ]
    for copy in keep + loads:
        copy.start()
    pl.semaphore_wait(barrier, owners + columns - 2)

    def parcel_copy(g, o):
        dest = lax.rem(me + o, owners)
        return pltpu.make_async_remote_copy(
            src_ref=staged[g].at[pl.ds(dest * slots, slots)],
            dst_ref=landed[g].at[mine],
            send_sem=send_sem.at[g, o],
            recv_sem=recv_sem.at[g, o],
            device_id={"grp": dest},
            device_id_type=MESH,
        )

    for g in range(group_count):
        for o in offsets:
            parcel_copy(g, o).start()

    for copy in keep + loads:
        copy.wait()

    dot_cols = min(256, block_len)
    rows_per = replicas
    chunk = partial.shape[1]

    for g, times in enumerate(TIME_GROUPS):
        for o in offsets:
            parcel_copy(g, o).wait_recv()
        rows = len(times) * rows_per
        base = times[0] * rows_per

        for k in range(tiles):
            piece = landed[g][own_place[k]]
            lhs[:rows, k * piece_len : (k + 1) * piece_len] = piece.reshape(rows, piece_len)

        def multiply(tile, carry):
            cols = pl.ds(pl.multiple_of(tile * dot_cols, dot_cols), dot_cols)
            coupled[base : base + rows, cols] = jnp.dot(
                lhs[:rows, :], weights[:, cols], preferred_element_type=jnp.float32
            )
            return carry

        lax.fori_loop(0, block_len // dot_cols, multiply, 0)

        steps = [t - 1 for t in times if t > 0]

        def move(tile, carry):
            cols = pl.ds(pl.multiple_of(tile * piece_len, piece_len), piece_len)
            y = [state[i, :, cols] for i in range(6)]
            drive = noise[:, cols]
            now = coupled[steps[0] * rows_per : (steps[0] + 1) * rows_per, cols]
            for i, s in enumerate(steps):
                later = coupled[(s + 1) * rows_per : (s + 2) * rows_per, cols]
                y = advance(y, drive, now, later)
                now = later
                potential[i * rows_per : (i + 1) * rows_per, cols] = (y[1] - y[2]).astype(
                    jnp.bfloat16
                )
            for i in range(6):
                state[i, :, cols] = y[i]
            return carry

        lax.fori_loop(0, block_len // piece_len, move, 0)

        if g == group_count - 1:
            save_state = pltpu.make_async_copy(state, final_hbm, local_sem.at[4])
            save_state.start()

        signal = lax.dot_general(
            potential[: len(steps) * rows_per, :],
            lead[...],
            (((1,), (1,)), ((), ())),
            preferred_element_type=jnp.float32,
        )
        row = steps[0] * rows_per
        stop = row + len(steps) * rows_per
        first_row = row
        while row < stop:
            part, inside = divmod(row, chunk)
            many = min(chunk - inside, stop - row)
            partial[part, inside : inside + many, :] = signal[
                row - first_row : row - first_row + many, :
            ]
            row += many

    def scatter_copy(o):
        dest = lax.rem(me + o, owners)
        return pltpu.make_async_remote_copy(
            src_ref=partial.at[dest],
            dst_ref=scatter_in.at[o],
            send_sem=scatter_send.at[o],
            recv_sem=scatter_recv.at[o],
            device_id={"grp": dest},
            device_id_type=MESH,
        )

    for o in offsets:
        scatter_copy(o).start()
    for g in range(group_count):
        for o in offsets:
            parcel_copy(g, o).wait_send()
    total = partial[me]
    for o in reversed(offsets):
        scatter_copy(o).wait_recv()
        total = total + scatter_in[o]
    node_in[column] = total

    def node_copy(o):
        return pltpu.make_async_remote_copy(
            src_ref=node_in.at[column],
            dst_ref=node_in.at[column],
            send_sem=node_send.at[o],
            recv_sem=node_recv.at[o],
            device_id={"node": lax.rem(column + o, columns)},
            device_id_type=MESH,
        )

    for o in range(1, columns):
        node_copy(o).start()
    for o in range(1, columns):
        node_copy(o).wait_recv()
    total = node_in[0]
    for c in range(1, columns):
        total = total + node_in[c]
    gathered[me] = total

    def gather_copy(o):
        return pltpu.make_async_remote_copy(
            src_ref=gathered.at[me],
            dst_ref=gathered.at[me],
            send_sem=gather_send.at[o],
            recv_sem=gather_recv.at[o],
            device_id={"grp": lax.rem(me + o, owners)},
            device_id_type=MESH,
        )

    for o in offsets:
        gather_copy(o).start()
    for o in offsets:
        scatter_copy(o).wait_send()
    for o in range(1, columns):
        node_copy(o).wait_send()
    for o in offsets:
        gather_copy(o).wait_recv()
    sensors_out[...] = gathered[...]
    for o in offsets:
        gather_copy(o).wait_send()
    save_state.wait()


def body(
    owners,
    columns,
    initial,
    afferent_noise_level,
    history,
    weights,
    lead_field,
    src_group,
    src_sub,
    delays,
    counts,
):
    cycle_len, replicas, block_len = history.shape
    tiles = src_group.shape[1]
    piece_len = weights.shape[2]
    sensors = lead_field.shape[0]
    slots = (tiles + owners - 1) // owners
    chunk = (STEPS * replicas + owners - 1) // owners
    groups = len(TIME_GROUPS)
    most = max(len(times) for times in TIME_GROUPS) * replicas
    smem = pl.BlockSpec(memory_space=pltpu.SMEM)
    vmem = pl.BlockSpec(memory_space=pltpu.VMEM)
    anywhere = pl.BlockSpec(memory_space=pl.ANY)
    own_place, *packed = pl.pallas_call(
        functools.partial(pack_kernel, owners, columns, slots),
        out_shape=[jax.ShapeDtypeStruct((tiles,), jnp.int32)]
        + [
            jax.ShapeDtypeStruct(
                (owners * slots, len(times), replicas, piece_len), jnp.bfloat16
            )
            for times in TIME_GROUPS
        ],
        in_specs=[smem] * 4 + [anywhere] * 2,
        out_specs=[smem] + [vmem] * groups,
        scratch_shapes=[
            pltpu.SMEM((owners * slots,), jnp.int32),
            pltpu.SMEM((owners * slots,), jnp.int32),
            pltpu.VMEM((replicas, block_len), jnp.bfloat16),
            pltpu.VMEM((2, replicas, block_len), jnp.float32),
            pltpu.VMEM(history.shape, jnp.bfloat16),
            pltpu.SemaphoreType.DMA((2,)),
        ],
        compiler_params=pltpu.CompilerParams(vmem_limit_bytes=VMEM_BYTES),
        cost_estimate=pl.CostEstimate(flops=0, bytes_accessed=8 * 1024 * 1024, transcendentals=0),
    )(src_group.T, src_sub.T, delays.T, counts, initial, history)
    final, signal = pl.pallas_call(
        functools.partial(kernel, owners, columns, slots),
        out_shape=(
            jax.ShapeDtypeStruct(initial.shape, jnp.float32),
            jax.ShapeDtypeStruct((owners, chunk, sensors), jnp.float32),
        ),
        in_specs=[smem] + [anywhere] * (4 + groups),
        out_specs=(anywhere, vmem),
        scratch_shapes=[
            pltpu.VMEM(initial.shape, jnp.float32),
            pltpu.VMEM((replicas, block_len), jnp.float32),
            pltpu.VMEM((tiles * piece_len, block_len), jnp.bfloat16),
            pltpu.VMEM(lead_field.shape, jnp.bfloat16),
            pltpu.VMEM((most, tiles * piece_len), jnp.bfloat16),
            pltpu.VMEM(((STEPS + 1) * replicas, block_len), jnp.float32),
            pltpu.VMEM((most, block_len), jnp.bfloat16),
            pltpu.VMEM((owners, chunk, sensors), jnp.float32),
            pltpu.VMEM((owners, chunk, sensors), jnp.float32),
            pltpu.VMEM((columns, chunk, sensors), jnp.float32),
            pltpu.VMEM((owners, chunk, sensors), jnp.float32),
            pltpu.SemaphoreType.DMA((5,)),
            pltpu.SemaphoreType.DMA((groups,)),
            pltpu.SemaphoreType.DMA((groups,)),
            pltpu.SemaphoreType.DMA((groups, owners)),
            pltpu.SemaphoreType.DMA((groups, owners)),
            pltpu.SemaphoreType.DMA((owners,)),
            pltpu.SemaphoreType.DMA((owners,)),
            pltpu.SemaphoreType.DMA((columns,)),
            pltpu.SemaphoreType.DMA((columns,)),
            pltpu.SemaphoreType.DMA((owners,)),
            pltpu.SemaphoreType.DMA((owners,)),
        ]
        + [
            pltpu.VMEM((owners * slots, len(times), replicas, piece_len), jnp.bfloat16)
            for times in TIME_GROUPS
        ]
        + [
            pltpu.VMEM((owners * slots + 1, len(times), replicas, piece_len), jnp.bfloat16)
            for times in TIME_GROUPS
        ],
        compiler_params=pltpu.CompilerParams(
            collective_id=0, has_side_effects=True, vmem_limit_bytes=VMEM_BYTES
        ),
    )(
        own_place,
        initial,
        afferent_noise_level,
        weights.reshape(tiles * piece_len, block_len),
        lead_field,
        *packed,
    )
    signal = signal.reshape(owners * chunk, sensors)[: STEPS * replicas]
    signal = signal.reshape(STEPS, replicas, sensors)
    return final, jnp.transpose(signal, (0, 2, 1))


def solution(mesh):
    return jax.shard_map(
        functools.partial(body, mesh.shape["grp"], mesh.shape["node"]),
        mesh=mesh,
        in_specs=(
            P(None, None, ("grp", "node")),
            P(None, ("grp", "node")),
            P(None, None, ("grp", "node")),
            P(("grp", "node"), None, None, None),
            P(None, ("grp", "node")),
            P(),
            P(),
            P(),
            P(),
        ),
        out_specs=(P(None, None, ("grp", "node")), P()),
        check_vma=False,
    )
```
